32 devices in a mesh: dp: 16 (over z, y, x), outer: 2 (over core).
Axes of the slice: x: 2, y: 2, z: 4, core: 2. Of those that a mesh axis runs over, the one named last changes fastest.
Arguments:
- gradient: float32 [32, 131072], P(('dp', 'outer')), may hold values from -6 to 6
- residual: float32 [32, 131072], P(('dp', 'outer')), may hold values from -6 to 6
- indices: int32 [32, 512], P(('dp', 'outer')), may hold values from 0 to 131071, as said below
- params: float32 [131072], replicated, may hold values from -6 to 6
Outputs:
- new_params: float32 [131072], replicated
- new_residual: float32 [32, 131072], P(('dp', 'outer'))
The draws below stay inside these ranges and needn't reach their ends.
Inputs may be any that keep to these rules, and one draw needn't show every extreme that they name: Within each worker's row the 512 indices are distinct and increasing: index j lies in [j * 256, (j + 1) * 256). Different workers often pick the same coordinate.
All inputs are finite; a program needn't handle non-finite values.
Results may differ from the reference program's by a relative error of at most 0.0003.
Values sent between devices are 32-bit elements.
A program may use at most 64 MiB of HBM per device.

```python
import jax
import jax.numpy as jnp

PARAMS = 131072
DENSITY = 256
KEEP = 512
WORKERS = 32


def draw_indices(key, part):
    shared = jax.random.randint(jax.random.fold_in(key, 11), (1, KEEP), 0, DENSITY)
    others = jax.random.randint(jax.random.fold_in(key, 12), (WORKERS, KEEP), 0, DENSITY)
    picker = jax.random.randint(jax.random.fold_in(key, 13), (WORKERS, KEEP), 0, 4)
    offsets = jnp.where(picker == 0, shared, others)
    blocks = jnp.arange(KEEP, dtype=jnp.int32)[None, :] * DENSITY
    return (blocks + offsets).astype(jnp.int32)


def block_scale(rng, extent, shards, smallest, high):
    level, own = 1.0, jax.random.fold_in(rng, 6)
    for axis_at, parts in shards:
        draws = jnp.exp(jax.random.uniform(jax.random.fold_in(own, axis_at), (parts,), jnp.float32, smallest / len(shards), high / len(shards)))
        level = level * jnp.repeat(draws, extent[axis_at] // parts).reshape([-1 if axis == axis_at else 1 for axis in range(len(extent))])
    return level


def normal_values(key, extent, spread, most, pieces=(), held_as=jnp.bfloat16):
    gain = block_scale(key, extent, pieces, -0.22, 0.18) if pieces else 1.0
    result = jax.random.normal(key, extent, jnp.float32) * spread * gain
    return jnp.minimum(jnp.maximum(result, -most), most).astype(held_as)


def setup_inputs(seed: int = 0) -> dict:
    key_of = jax.random.split(jax.random.key(seed), 5)
    return {
        "gradient": normal_values(key_of[0], (WORKERS, PARAMS), 1.0, 6.0, ((0, 32),), jnp.float32),
        "residual": normal_values(key_of[1], (WORKERS, PARAMS), 0.5, 6.0, ((0, 32),), jnp.float32),
        "indices": draw_indices(jax.random.fold_in(key_of[4], 71), 0),
        "params": normal_values(key_of[3], (PARAMS,), 1.0, 6.0, (), jnp.float32),
    }


def reference(gradient, residual, indices, params):
    accumulated = gradient + residual
    sent = jnp.take_along_axis(accumulated, indices, axis=1)
    total = jnp.zeros((PARAMS,), jnp.float32).at[indices.reshape(-1)].add(sent.reshape(-1))
    new_params = params - 0.5 * total
    worker_rows = jnp.arange(WORKERS, dtype=jnp.int32)[:, None]
    new_residual = accumulated.at[worker_rows, indices].set(jnp.float32(0.0))
    return new_params, new_residual
```

```python
import functools

import jax
import jax.numpy as jnp
from jax import lax
from jax.experimental import pallas as pl
from jax.experimental.pallas import tpu as pltpu
from jax.sharding import PartitionSpec as P

MESH = pl.DeviceIdType.MESH
step_size = 0.5
LANES = 128
GROUPS = 4
CHUNK = 8
STRIP = 64


def kernel(n, outer, gradient, residual, indices, total, kept,
           grad_v, resid_v, index_v, pairs, turned, partial,
           in_sem, send_sem, recv_sem):
    tiles = indices.shape[0]
    block = gradient.shape[0] // tiles
    halves = block // LANES
    me = lax.axis_index("dp") * outer + lax.axis_index("outer")

    def at(worker):
        return (worker // outer, lax.rem(worker, outer))

    loads = [pltpu.make_async_copy(indices, index_v, in_sem.at[2 * tiles])]
    for t in range(tiles):
        rows = pl.ds(t * block, block)
        loads.append(pltpu.make_async_copy(gradient.at[rows], grad_v.at[rows], in_sem.at[2 * t]))
        loads.append(pltpu.make_async_copy(residual.at[rows], resid_v.at[rows], in_sem.at[2 * t + 1]))
    for load in loads:
        load.start()

    barrier = pltpu.get_barrier_semaphore()

    def greet(k, carry):
        pl.semaphore_signal(barrier, inc=1, device_id=at(lax.rem(me + k, n)), device_id_type=MESH)
        return carry

    lax.fori_loop(1, n, greet, 0)

    loads[0].wait()
    blocks = (lax.broadcasted_iota(jnp.int32, index_v.shape, 0) * LANES
              + lax.broadcasted_iota(jnp.int32, index_v.shape, 1))
    offsets = (index_v[...] - blocks * (halves * LANES)).astype(jnp.float32)
    row_at = lax.broadcasted_iota(jnp.int32, (LANES, LANES), 0).astype(jnp.float32)

    def chosen(t, h):
        return offsets[t:t + 1, :] - jnp.float32(h * LANES) == row_at

    sent = []
    for t in range(tiles):
        loads[1 + 2 * t].wait()
        loads[2 + 2 * t].wait()
        mine = jnp.zeros((1, LANES), jnp.float32)
        for h in range(halves):
            rows = pl.ds(t * block + h, LANES, stride=halves)
            flipped = (grad_v[rows, :] + resid_v[rows, :]).T
            turned[h * LANES:(h + 1) * LANES, t * LANES:(t + 1) * LANES] = flipped
            mine += jnp.sum(jnp.where(chosen(t, h), flipped, 0.0), axis=0, keepdims=True)
        sent.append(mine)
    pairs[me] = jnp.concatenate(sent + [offsets], axis=0)

    pl.semaphore_wait(barrier, n - 1)

    def copy_to(worker):
        return pltpu.make_async_remote_copy(
            src_ref=pairs.at[me], dst_ref=pairs.at[me],
            send_sem=send_sem.at[worker], recv_sem=recv_sem.at[me],
            device_id=at(worker), device_id_type=MESH)

    def copy_from(worker):
        return pltpu.make_async_remote_copy(
            src_ref=pairs.at[me], dst_ref=pairs.at[worker],
            send_sem=send_sem.at[worker], recv_sem=recv_sem.at[worker],
            device_id=at(worker), device_id_type=MESH)

    def send(k, carry):
        worker = lax.rem(me + n // 2 + k, n)

        @pl.when(worker != me)
        def _():
            copy_to(worker).start()

        return carry

    lax.fori_loop(0, n, send, 0)

    for t in range(tiles):
        for h in range(halves):
            flipped = turned[h * LANES:(h + 1) * LANES, t * LANES:(t + 1) * LANES]
            rows = pl.ds(t * block + h, LANES, stride=halves)
            kept[rows, :] = jnp.where(chosen(t, h), 0.0, flipped).T

    size = n // GROUPS
    strip_at = lax.broadcasted_iota(jnp.int32, (STRIP, LANES), 0).astype(jnp.float32)
    my_group = me // size

    def add_group(i, carry):
        away = jnp.where(i == 2, 3, jnp.where(i == 3, 2, i))
        group = lax.rem(my_group + away, GROUPS)

        def arrived(k, carry):
            worker = group * size + k

            @pl.when(worker != me)
            def _():
                copy_from(worker).wait_recv()

            return carry

        lax.fori_loop(0, size, arrived, 0)
        for first in range(0, size, CHUNK):
            many = min(CHUNK, size - first)
            for t in range(tiles):
                lanes = slice(t * LANES, (t + 1) * LANES)
                for s in range(0, halves * LANES, STRIP):
                    strip = (group, slice(s, s + STRIP), lanes)
                    added = None
                    for k in range(many):
                        pair = pairs.at[group * size + first + k]
                        hit = pair[tiles + t:tiles + t + 1, :] - jnp.float32(s) == strip_at
                        value = jnp.where(hit, pair[t:t + 1, :], 0.0)
                        added = value if added is None else added + value
                    if first:
                        added = added + partial[strip]
                    partial[strip] = added
        return carry

    lax.fori_loop(0, GROUPS, add_group, 0)

    for t in range(tiles):
        for h in range(halves):
            piece = (slice(h * LANES, (h + 1) * LANES), slice(t * LANES, (t + 1) * LANES))
            summed = partial[(0,) + piece]
            for group in range(1, GROUPS):
                summed = summed + partial[(group,) + piece]
            rows = pl.ds(t * block + h, LANES, stride=halves)
            total[rows, :] = summed.T

    def sent_off(k, carry):
        copy_to(lax.rem(me + k, n)).wait_send()
        return carry

    lax.fori_loop(1, n, sent_off, 0)


def shards(n, outer, gradient, residual, indices, params):
    width, keep = gradient.shape[1], indices.shape[1]
    tiles, block = keep // LANES, width // keep
    long = (width // LANES, LANES)
    any_space = pl.BlockSpec(memory_space=pl.ANY)
    vmem = pl.BlockSpec(memory_space=pltpu.VMEM)
    total, kept = pl.pallas_call(
        functools.partial(kernel, n, outer),
        out_shape=[jax.ShapeDtypeStruct(long, jnp.float32)] * 2,
        in_specs=[any_space] * 3,
        out_specs=[vmem] * 2,
        scratch_shapes=[
            pltpu.VMEM(long, jnp.float32),
            pltpu.VMEM(long, jnp.float32),
            pltpu.VMEM((tiles, LANES), jnp.int32),
            pltpu.VMEM((n, 2 * tiles, LANES), jnp.float32),
            pltpu.VMEM((block, keep), jnp.float32),
            pltpu.VMEM((GROUPS, block, keep), jnp.float32),
            pltpu.SemaphoreType.DMA((2 * tiles + 1,)),
            pltpu.SemaphoreType.DMA((n,)),
            pltpu.SemaphoreType.DMA((n,)),
        ],
        compiler_params=pltpu.CompilerParams(collective_id=0, has_side_effects=True),
    )(gradient.reshape(long), residual.reshape(long), indices.reshape(tiles, LANES))
    new_params = params - step_size * total.reshape(width)
    return new_params, kept.reshape(1, width)


def solution(mesh):
    outer = mesh.shape["outer"]
    n = mesh.shape["dp"] * outer
    placed = (P(("dp", "outer"), None), P(("dp", "outer"), None), P(("dp", "outer"), None), P())
    return jax.shard_map(
        functools.partial(shards, n, outer),
        mesh=mesh,
        in_specs=placed,
        out_specs=(P(), P(("dp", "outer"), None)),
        check_vma=False,
    )
```
